32 devices in a mesh: views: 2 (over x), depth: 16 (over z, y, core).
Axes of the slice: x: 2, y: 2, z: 4, core: 2. Of those that a mesh axis runs over, the one named last changes fastest.
Arguments:
- density: float32 [512, 128, 256], P(('views', 'depth')), parts along dimension 0, may hold values from 0.2 to 5
- emission: bfloat16 [6, 256, 128, 256], P('views', 'depth'), parts along dimension 0, may hold values from 0 to 1
- occupancy: int32 [32, 4, 4], P(('views', 'depth')), parts along dimension 0, may hold values 0 or 1
- facing: int32 [2], P('views'), parts along dimension 0, may hold values from 0 to 1
Outputs:
- image: float32 [8, 128, 256], P('views', 'depth'), parts along dimension 0
The draws below stay inside these ranges and needn't reach their ends.
There are 2 independent parts, one for each index of `views`. The reference program is written for one: setup_inputs(seed, part) draws one part's arguments, and reference() takes and returns one part's arrays. A program takes and returns all parts, laid end to end along the dimension named above; each array names one. Nothing has to cross between parts.
Inputs may be any that keep to these rules, and one draw needn't show every extreme that they name: `occupancy`: 1 where the tile of the brick is occupied; where it is 0 the tile's cells neither absorb nor emit. `facing`: 0: bricks and cells of lower depth index are nearer the camera; 1: those of higher index.
All inputs are finite; a program needn't handle non-finite values. No bound on the sum of `occupancy` on one device may be relied on, other than what follows from the above.
Results may differ from the reference program's by a relative error of at most 0.0003.
Values sent between devices are 32-bit elements; how exact they have to be, the bound alone decides.
No kernel may reach another device: no remote copies, remote signals or barrier semaphores. Data moves between devices by JAX's collectives and lax.ppermute only.
A program may use at most 128 MiB of HBM per device.

```python
import math
import jax
import jax.numpy as jnp
from jax import lax

IMG_H = 128
IMG_W = 256
DEPTH_DEV = 16
BRICKS = 16
NZ = 256
TILES_H = 4
TILES_W = 4
N_DEPTH = 16


def plant(values, rng, smallest, top_value):
    longest = values.shape.index(max(values.shape))
    spots = []
    for shift in (0, 1):
        where = [jax.random.randint(jax.random.fold_in(rng, axis), (), 0, length) for axis, length in enumerate(values.shape)]
        where[longest] = (where[longest] + shift) % values.shape[longest]
        spots.append(tuple(where))
    return values.at[spots[0]].set(smallest).at[spots[1]].set(top_value)


def block_levels(stream_key, dims, shards, smallest, top_value):
    factor_of = 1.0
    for position, parts in shards:
        heights = jax.random.uniform(jax.random.fold_in(jax.random.fold_in(stream_key, 6), position), (parts,), jnp.float32, smallest / len(shards), top_value / len(shards))
        factor_of = factor_of * jnp.repeat(jnp.exp(heights), dims[position] // parts).reshape((-1,) + (1,) * (len(dims) - 1 - position))
    return factor_of


def setup_inputs(seed: int = 0, part: int = 0) -> dict:
    arg_keys = jax.random.split(jax.random.key(seed), 5)
    own_keys = jax.random.split(jax.random.fold_in(arg_keys[4], part), 5)
    density = jnp.clip(jnp.exp(math.log(5.0) - 3.218876 * jax.random.uniform(own_keys[0], (NZ, IMG_H, IMG_W), jnp.float32) ** block_levels(own_keys[0], (NZ, IMG_H, IMG_W), ((0, 16),), -0.2, 0.2)), 0.2, 5.0)
    emission = jnp.clip(1.0 * jax.random.uniform(own_keys[1], (3, NZ, IMG_H, IMG_W), jnp.float32) ** block_levels(own_keys[1], (3, NZ, IMG_H, IMG_W), ((1, 16),), -0.2, 0.2), 0.0, 1.0).astype(jnp.bfloat16)
    occupancy = plant((jax.random.randint(own_keys[2], (BRICKS, TILES_H, TILES_W), 0, 4) < 3).astype(jnp.int32), jax.random.fold_in(own_keys[2], 1), 0, 1)
    facing = jax.random.randint(own_keys[3], (1,), 0, 2).astype(jnp.int32)
    return dict(density=density, emission=emission, occupancy=occupancy, facing=facing)


def march(dense, emitted, occupied, facing, bricks):
    depth_len, height, width = dense.shape
    tiles_h, tiles_w = occupied.shape
    gating = occupied.astype(jnp.float32)[None, :, None, :, None]
    optical = (dense.reshape(depth_len, tiles_h, height // tiles_h, tiles_w, width // tiles_w) * gating).reshape(dense.shape) / (depth_len * bricks)
    column = jnp.cumsum(optical, axis=0)
    whole = column[-1]
    ahead = jnp.where(facing == 0, column - optical, whole[None] - column)
    weight = (1.0 - jnp.exp(-optical)) * jnp.exp(-ahead)
    radiance = jnp.sum(emitted.astype(jnp.float32) * weight[None], axis=1)
    return radiance, jnp.exp(-whole)


def composite(radiance, transmit, facing):
    ones_row = jnp.ones_like(transmit[:1])
    forward = jnp.cumprod(transmit, axis=0)
    ahead_forward = jnp.concatenate([ones_row, forward[:-1]], axis=0)
    backward = jnp.flip(jnp.cumprod(jnp.flip(transmit, 0), axis=0), 0)
    ahead_backward = jnp.concatenate([backward[1:], ones_row], axis=0)
    front = jnp.where(facing == 0, ahead_forward, ahead_backward)
    colour = jnp.sum(radiance * front, axis=0)
    opacity = 1.0 - forward[-1]
    return jnp.concatenate([colour, opacity], axis=0)


def reference(density, emission, occupancy, facing):
    def single(brick_index):
        dense = lax.dynamic_slice_in_dim(density, brick_index * DEPTH_DEV, DEPTH_DEV, 0)
        emitted = lax.dynamic_slice_in_dim(emission, brick_index * DEPTH_DEV, DEPTH_DEV, 1)
        occupied = lax.dynamic_index_in_dim(occupancy, brick_index, 0, keepdims=False)
        return march(dense, emitted, occupied, facing[0], N_DEPTH)

    radiance, transmit = lax.map(single, jnp.arange(N_DEPTH, dtype=jnp.int32))
    return composite(radiance, transmit[:, None], facing[0])
```

```python
import functools
import math

import jax
import jax.numpy as jnp
from jax import lax
from jax.experimental import pallas as pl
from jax.experimental.pallas import tpu as pltpu
from jax.sharding import PartitionSpec as P

ROWS = 8


def march_body(sel, facing, occupied, dense, emitted, out, dense_buf, emitted_buf, dense_sem, emitted_sem, *, chunks, tile_rows, bricks):
    depth_len, pairs, _, rows, width = dense.shape
    tiles_h, tiles_w = occupied.shape
    per = pairs // chunks
    half = sel[0]
    backward = facing[0] != 0

    def copies(chunk):
        span = pl.ds(chunk * per, per)
        return (
            pltpu.make_async_copy(dense.at[:, span, half], dense_buf.at[:, span], dense_sem.at[chunk]),
            pltpu.make_async_copy(emitted.at[:, :, span, half], emitted_buf.at[:, :, span], emitted_sem.at[chunk]),
        )

    for chunk in range(chunks):
        for copy in copies(chunk):
            copy.start()

    lane = lax.broadcasted_iota(jnp.int32, (ROWS, width), 1) // (width // tiles_w)
    scale = -math.log2(math.e) / (depth_len * bricks)

    for chunk in range(chunks):
        for copy in copies(chunk):
            copy.wait()

        def group(index, _, chunk=chunk):
            pair = chunk * per + index // (rows // ROWS)
            sub = index % (rows // ROWS)
            first = (pair * 2 + half) * rows + sub * ROWS
            tile = first // tile_rows
            gate = jnp.zeros((ROWS, width), jnp.float32)
            for column in range(tiles_w):
                gate = jnp.where(lane == column, occupied[tile, column].astype(jnp.float32) * scale, gate)
            span = pl.ds(pl.multiple_of(sub * ROWS, ROWS), ROWS)
            total = jnp.zeros((ROWS, width), jnp.float32)
            before = jnp.ones((ROWS, width), jnp.float32)
            colour = [jnp.zeros((ROWS, width), jnp.float32) for _ in range(3)]
            for step in range(depth_len):
                cell = jnp.where(backward, depth_len - 1 - step, step)
                total = total + dense_buf[cell, pair, span, :]
                after = jnp.exp2(total * gate)
                weight = before - after
                before = after
                for channel in range(3):
                    colour[channel] = colour[channel] + emitted_buf[channel, cell, pair, span, :].astype(jnp.float32) * weight
            for channel in range(3):
                out[pair, sub, channel] = colour[channel]
            out[pair, sub, 3] = before
            return 0

        lax.fori_loop(0, per * (rows // ROWS), group, 0)


def march(dense, emitted, occupied, facing, half, bricks):
    depth_len, pairs, _, rows, width = dense.shape
    tile_rows = pairs * 2 * rows // occupied.shape[0]
    chunks = math.gcd(pairs, 4)
    smem = pl.BlockSpec(memory_space=pltpu.SMEM)
    hbm = pl.BlockSpec(memory_space=pl.ANY)
    return pl.pallas_call(
        functools.partial(march_body, chunks=chunks, tile_rows=tile_rows, bricks=bricks),
        in_specs=[smem, smem, smem, hbm, hbm],
        out_specs=pl.BlockSpec(memory_space=pltpu.VMEM),
        out_shape=jax.ShapeDtypeStruct((pairs, rows // ROWS, 4, ROWS, width), jnp.float32),
        scratch_shapes=[
            pltpu.VMEM((depth_len, pairs, rows, width), jnp.float32),
            pltpu.VMEM((3, depth_len, pairs, rows, width), jnp.bfloat16),
            pltpu.SemaphoreType.DMA((chunks,)),
            pltpu.SemaphoreType.DMA((chunks,)),
        ],
        name="march",
    )(half, facing, occupied, dense, emitted)


def over(mine, other, nearer):
    colour, through = mine[..., :3, :, :], mine[..., 3:, :, :]
    colour_other, through_other = other[..., :3, :, :], other[..., 3:, :, :]
    merged = jnp.where(nearer, colour + through * colour_other, colour_other + through_other * colour)
    return jnp.concatenate([merged, through * through_other], axis=-3)


def swap(value, bit, size):
    return lax.ppermute(value, "depth", [(i, i ^ bit) for i in range(size)])


def halves(value, bit, place, axis):
    own = (place // bit) % 2
    keep = lax.dynamic_index_in_dim(value, own, axis, keepdims=False)
    give = lax.dynamic_index_in_dim(value, 1 - own, axis, keepdims=False)
    return keep, give


def on_device(density, emission, occupancy, facing):
    size = lax.axis_size("depth")
    place = lax.axis_index("depth")
    forward = facing[0] == 0
    depth_len, height, width = density.shape
    rows = height // size

    def nearer(bit):
        return ((place // bit) % 2 == 0) == forward

    own = (place % 2).astype(jnp.int32)
    if rows % ROWS == 0:
        pairs, unit = size // 2, rows
    else:
        pairs, unit = height // (2 * ROWS), ROWS
    dense = density.reshape(depth_len, pairs, 2, unit, width)
    emitted = emission.reshape(3, depth_len, pairs, 2, unit, width)
    if rows % ROWS == 0:
        give = march(dense, emitted, occupancy[0], facing, (1 - own)[None], size)
        got = swap(give, 1, size)
        keep = march(dense, emitted, occupancy[0], facing, own[None], size)
    else:
        both = jnp.stack([march(dense, emitted, occupancy[0], facing, jnp.full((1,), k, jnp.int32), size) for k in range(2)], axis=1)
        both = jnp.moveaxis(both[:, :, 0], 2, 0).reshape(4, size // 2, 2, 1, rows, width)
        both = jnp.moveaxis(both, 0, 3)
        keep, give = halves(both, 1, place, 1)
        got = swap(give, 1, size)
    value = over(keep, got, nearer(1))

    bit = 2
    while bit < size:
        tiles = value.shape[0]
        if bit == 2 and tiles >= 4:
            value = value.reshape((tiles // 4, 2, 2) + value.shape[1:])
            mine, theirs = halves(value, 2 * bit, place, 1)
            keep, give_low = halves(mine, bit, place, 1)
            give_high, give_both = halves(theirs, bit, place, 1)
            got_both = swap(give_both, 3 * bit, size)
            got_high = swap(give_high, 2 * bit, size)
            got_low = swap(give_low, bit, size)
            value = over(over(keep, got_low, nearer(bit)), over(got_high, got_both, nearer(bit)), nearer(2 * bit))
            bit *= 4
        else:
            value = value.reshape((tiles // 2, 2) + value.shape[1:])
            keep, give = halves(value, bit, place, 1)
            value = over(keep, swap(give, bit, size), nearer(bit))
            bit *= 2
    value = jnp.moveaxis(value[0], 1, 0).reshape(4, rows, width)
    return jnp.concatenate([value[:3], 1.0 - value[3:]], axis=0)


def solution(mesh):
    return jax.shard_map(
        on_device,
        mesh=mesh,
        in_specs=(
            P(("views", "depth"), None, None),
            P("views", "depth", None, None),
            P(("views", "depth"), None, None),
            P("views"),
        ),
        out_specs=P("views", "depth", None),
        check_vma=False,
    )
```

```python
import functools
import math

import jax
import jax.numpy as jnp
from jax import lax
from jax.experimental import pallas as pl
from jax.experimental.pallas import tpu as pltpu
from jax.sharding import PartitionSpec as P

ROWS = 8
CROSSING = ~4


def parity(chip_bits):
    for shift in (8, 4, 2, 1):
        chip_bits = chip_bits ^ (chip_bits >> shift)
    return chip_bits & 1


def side(pair):
    return parity((pair * 2) & CROSSING & 0xFFFE)


def march_body(facing, occupied_hbm, dense, emitted, out, dense_buf, emitted_buf, occupied, dense_sem, emitted_sem, small_sem, *, other, tile_rows, bricks):
    depth_len, pairs, _, rows, width = dense.shape
    tiles_h, tiles_w = occupied.shape
    place = lax.axis_index("depth")
    chosen = ((place & 1) ^ side(place >> 1)) ^ int(other)

    small = pltpu.make_async_copy(occupied_hbm, occupied, small_sem)
    small.start()

    def copies(pair):
        half = chosen ^ side(pair)
        return (
            pltpu.make_async_copy(dense.at[:, pair, half], dense_buf.at[:, pair], dense_sem.at[pair]),
            pltpu.make_async_copy(emitted.at[:, :, pair, half], emitted_buf.at[:, :, pair], emitted_sem.at[pair]),
        )

    for pair in range(pairs):
        for copy in copies(pair):
            copy.start()

    lane = lax.broadcasted_iota(jnp.int32, (ROWS, width), 1) // (width // tiles_w)
    scale = -math.log2(math.e) / (depth_len * bricks)
    small.wait()
    backward = facing[0] != 0

    def march_pair(pair, _):
        for copy in copies(pair):
            copy.wait()
        half = chosen ^ side(pair)
        for sub in range(rows // ROWS):
            tile = ((pair * 2 + half) * rows + sub * ROWS) // tile_rows
            gate = jnp.zeros((ROWS, width), jnp.float32)
            for column in range(tiles_w):
                gate = jnp.where(lane == column, occupied[tile, column].astype(jnp.float32) * scale, gate)
            span = pl.ds(sub * ROWS, ROWS)
            total = jnp.zeros((ROWS, width), jnp.float32)
            before = jnp.ones((ROWS, width), jnp.float32)
            colour = [jnp.zeros((ROWS, width), jnp.float32) for _ in range(3)]
            for step in range(depth_len):
                cell = jnp.where(backward, depth_len - 1 - step, step)
                total = total + dense_buf[cell, pair, span, :]
                after = jnp.exp2(total * gate)
                weight = before - after
                before = after
                for channel in range(3):
                    colour[channel] = colour[channel] + emitted_buf[channel, cell, pair, span, :].astype(jnp.float32) * weight
            for channel in range(3):
                out[pair, sub, channel] = colour[channel]
            out[pair, sub, 3] = before
        return 0

    lax.fori_loop(0, pairs, march_pair, 0)


def march(dense, emitted, occupied, facing, other, bricks):
    depth_len, pairs, _, rows, width = dense.shape
    tile_rows = pairs * 2 * rows // occupied.shape[0]
    hbm = pl.BlockSpec(memory_space=pl.ANY)
    return pl.pallas_call(
        functools.partial(march_body, other=other, tile_rows=tile_rows, bricks=bricks),
        in_specs=[pl.BlockSpec(memory_space=pltpu.SMEM), hbm, hbm, hbm],
        out_specs=pl.BlockSpec(memory_space=pltpu.VMEM),
        out_shape=pltpu.VMEM((pairs, rows // ROWS, 4, ROWS, width), jnp.float32),
        scratch_shapes=[
            pltpu.VMEM((depth_len, pairs, rows, width), jnp.float32),
            pltpu.VMEM((3, depth_len, pairs, rows, width), jnp.bfloat16),
            pltpu.SMEM(occupied.shape, jnp.int32),
            pltpu.SemaphoreType.DMA((pairs,)),
            pltpu.SemaphoreType.DMA((pairs,)),
            pltpu.SemaphoreType.DMA,
        ],
        name="march",
    )(facing, occupied, dense, emitted)


def over(mine, other, nearer):
    colour, through = mine[..., :3, :, :], mine[..., 3:, :, :]
    colour_other, through_other = other[..., :3, :, :], other[..., 3:, :, :]
    merged = jnp.where(nearer, colour + through * colour_other, colour_other + through_other * colour)
    return jnp.concatenate([merged, through * through_other], axis=-3)


def swap(value, mask, size):
    mask = mask | parity(mask & CROSSING & 0xFFFE)
    return lax.ppermute(value, "depth", [(i, i ^ mask) for i in range(size)])


def halves(value, bit, place):
    own = jnp.minimum(place & bit, 1)
    keep = lax.dynamic_index_in_dim(value, own, 1, keepdims=False)
    give = lax.dynamic_index_in_dim(value, 1 - own, 1, keepdims=False)
    return keep, give


def on_device(density, emission, occupancy, facing):
    size = lax.axis_size("depth")
    place = lax.axis_index("depth")
    depth_len, height, width = density.shape
    rows = height // size
    aligned = rows % ROWS == 0
    pairs, unit = (size // 2, rows) if aligned else (height // (2 * ROWS), ROWS)
    dense = density.reshape(depth_len, pairs, 2, unit, width)
    emitted = emission.reshape(3, depth_len, pairs, 2, unit, width)

    give = march(dense, emitted, occupancy[0], facing, True, size)
    keep = march(dense, emitted, occupancy[0], facing, False, size)
    if not aligned:
        pair = jnp.arange(pairs)
        chosen = ((place & 1) ^ side(place >> 1)) ^ side(pair)
        swapped = (chosen == 1)[:, None, None, None]
        both = jnp.stack([jnp.where(swapped, give[:, 0], keep[:, 0]), jnp.where(swapped, keep[:, 0], give[:, 0])], axis=1)
        both = jnp.moveaxis(both, 2, 0).reshape(4, size // 2, 2, 1, rows, width)
        both = jnp.moveaxis(both, 0, 3)
        pair = jnp.arange(size // 2)
        swapped = ((((place & 1) ^ side(place >> 1)) ^ side(pair)) == 1)[:, None, None, None, None]
        keep = jnp.where(swapped, both[:, 1], both[:, 0])
        give = jnp.where(swapped, both[:, 0], both[:, 1])
    forward = facing[0] == 0

    def nearer(bit):
        return ((place & bit) == 0) == forward

    value = over(keep, swap(give, 1, size), nearer(1))
    bit = 2
    while bit < size:
        tiles = value.shape[0]
        if bit == 2 and tiles >= 4:
            value = value.reshape((tiles // 4, 2, 2) + value.shape[1:])
            mine, theirs = halves(value, 2 * bit, place)
            keep, give_low = halves(mine, bit, place)
            give_high, give_both = halves(theirs, bit, place)
            got_both = swap(give_both, 3 * bit, size)
            got_high = swap(give_high, 2 * bit, size)
            got_low = swap(give_low, bit, size)
            value = over(over(keep, got_low, nearer(bit)), over(got_high, got_both, nearer(bit)), nearer(2 * bit))
            bit *= 4
        else:
            value = value.reshape((tiles // 2, 2) + value.shape[1:])
            keep, give = halves(value, bit, place)
            value = over(keep, swap(give, bit, size), nearer(bit))
            bit *= 2
    value = jnp.moveaxis(value[0], 1, 0).reshape(4, rows, width)
    return jnp.concatenate([value[:3], 1.0 - value[3:]], axis=0)


def solution(mesh):
    return jax.shard_map(
        on_device,
        mesh=mesh,
        in_specs=(
            P(("views", "depth"), None, None),
            P("views", "depth", None, None),
            P(("views", "depth"), None, None),
            P("views"),
        ),
        out_specs=P("views", "depth", None),
        check_vma=False,
    )
```

```python
import functools
import math

import jax
import jax.numpy as jnp
from jax import lax
from jax.experimental import pallas as pl
from jax.experimental.pallas import tpu as pltpu
from jax.sharding import PartitionSpec as P


ROWS = 8
CHUNKS = 8
CROSSING = ~4


def parity(chip_bits):
    for shift in (8, 4, 2, 1):
        chip_bits = chip_bits ^ (chip_bits >> shift)
    return chip_bits & 1


def side(pair):
    return parity((pair * 2) & CROSSING & 0xFFFE)


def march_body(facing, occupied_hbm, dense, emitted, keep, give, dense_buf, emitted_buf, occupied, dense_sem, emitted_sem, small_sem, *, chunks, tile_rows, bricks):
    depth_len, pairs, _, rows, width = dense.shape
    _, tiles_w = occupied.shape
    per = pairs // chunks
    place = lax.axis_index("depth")
    chosen = (place & 1) ^ side(place >> 1)

    small = pltpu.make_async_copy(occupied_hbm, occupied, small_sem)
    small.start()

    def copies(chunk):
        span = pl.ds(chunk * per, per)
        return (
            pltpu.make_async_copy(dense.at[:, span], dense_buf.at[:, span], dense_sem.at[chunk]),
            pltpu.make_async_copy(emitted.at[:, :, span], emitted_buf.at[:, :, span], emitted_sem.at[chunk]),
        )

    for chunk in range(chunks):
        for copy in copies(chunk):
            copy.start()

    lane = lax.broadcasted_iota(jnp.int32, (ROWS, width), 1) // (width // tiles_w)
    scale = -math.log2(math.e) / (depth_len * bricks)
    small.wait()
    backward = facing[0] != 0

    def march_chunk(chunk, _):
        for copy in copies(chunk):
            copy.wait()

        def march_pair(index, _):
            pair = chunk * per + index
            for other, out in ((0, keep), (1, give)):
                half = chosen ^ side(pair) ^ other
                for sub in range(rows // ROWS):
                    tile = ((pair * 2 + half) * rows + sub * ROWS) // tile_rows
                    gate = jnp.zeros((ROWS, width), jnp.float32)
                    for column in range(tiles_w):
                        gate = jnp.where(lane == column, occupied[tile, column].astype(jnp.float32) * scale, gate)
                    span = pl.ds(sub * ROWS, ROWS)
                    total = jnp.zeros((ROWS, width), jnp.float32)
                    before = jnp.ones((ROWS, width), jnp.float32)
                    colour = [jnp.zeros((ROWS, width), jnp.float32) for _ in range(3)]
                    for step in range(depth_len):
                        cell = jnp.where(backward, depth_len - 1 - step, step)
                        total = total + dense_buf[cell, pair, half, span, :]
                        after = jnp.exp2(total * gate)
                        weight = before - after
                        before = after
                        for channel in range(3):
                            colour[channel] = colour[channel] + emitted_buf[channel, cell, pair, half, span, :].astype(jnp.float32) * weight
                    for channel in range(3):
                        out[pair, sub, channel] = colour[channel]
                    out[pair, sub, 3] = before
            return 0

        lax.fori_loop(0, per, march_pair, 0)
        return 0

    lax.fori_loop(0, chunks, march_chunk, 0)


def march(dense, emitted, occupied, facing, bricks):
    _, pairs, _, rows, width = dense.shape
    tile_rows = pairs * 2 * rows // occupied.shape[0]
    chunks = math.gcd(pairs, CHUNKS)
    hbm = pl.BlockSpec(memory_space=pl.ANY)
    half = pltpu.VMEM((pairs, rows // ROWS, 4, ROWS, width), jnp.float32)
    return pl.pallas_call(
        functools.partial(march_body, chunks=chunks, tile_rows=tile_rows, bricks=bricks),
        in_specs=[pl.BlockSpec(memory_space=pltpu.SMEM), hbm, hbm, hbm],
        out_specs=(pl.BlockSpec(memory_space=pltpu.VMEM), pl.BlockSpec(memory_space=pltpu.VMEM)),
        out_shape=(half, half),
        scratch_shapes=[
            pltpu.VMEM(dense.shape, jnp.float32),
            pltpu.VMEM(emitted.shape, jnp.bfloat16),
            pltpu.SMEM(occupied.shape, jnp.int32),
            pltpu.SemaphoreType.DMA((chunks,)),
            pltpu.SemaphoreType.DMA((chunks,)),
            pltpu.SemaphoreType.DMA,
        ],
        name="march",
    )(facing, occupied, dense, emitted)


def over(mine, other, nearer):
    colour, through = mine[..., :3, :, :], mine[..., 3:, :, :]
    colour_other, through_other = other[..., :3, :, :], other[..., 3:, :, :]
    merged = jnp.where(nearer, colour + through * colour_other, colour_other + through_other * colour)
    return jnp.concatenate([merged, through * through_other], axis=-3)


def swap(value, mask, size):
    mask = mask | parity(mask & CROSSING & 0xFFFE)
    return lax.ppermute(value, "depth", [(i, i ^ mask) for i in range(size)])


def halves(value, bit, place):
    own = jnp.minimum(place & bit, 1)
    keep = lax.dynamic_index_in_dim(value, own, 1, keepdims=False)
    give = lax.dynamic_index_in_dim(value, 1 - own, 1, keepdims=False)
    return keep, give


def on_device(density, emission, occupancy, facing):
    size = lax.axis_size("depth")
    place = lax.axis_index("depth")
    depth_len, height, width = density.shape
    rows = height // size
    aligned = rows % ROWS == 0
    pairs, unit = (size // 2, rows) if aligned else (height // (2 * ROWS), ROWS)
    dense = density.reshape(depth_len, pairs, 2, unit, width)
    emitted = emission.reshape(3, depth_len, pairs, 2, unit, width)

    keep, give = march(dense, emitted, occupancy[0], facing, size)
    if not aligned:
        pair = jnp.arange(pairs)
        chosen = ((place & 1) ^ side(place >> 1)) ^ side(pair)
        swapped = (chosen == 1)[:, None, None, None]
        both = jnp.stack([jnp.where(swapped, give[:, 0], keep[:, 0]), jnp.where(swapped, keep[:, 0], give[:, 0])], axis=1)
        both = jnp.moveaxis(both, 2, 0).reshape(4, size // 2, 2, 1, rows, width)
        both = jnp.moveaxis(both, 0, 3)
        pair = jnp.arange(size // 2)
        swapped = ((((place & 1) ^ side(place >> 1)) ^ side(pair)) == 1)[:, None, None, None, None]
        keep = jnp.where(swapped, both[:, 1], both[:, 0])
        give = jnp.where(swapped, both[:, 0], both[:, 1])
    forward = facing[0] == 0

    def nearer(bit):
        return ((place & bit) == 0) == forward

    value = over(keep, swap(give, 1, size), nearer(1))
    bit = 2
    while bit < size:
        tiles = value.shape[0]
        if bit == 2 and tiles >= 4:
            value = value.reshape((tiles // 4, 2, 2) + value.shape[1:])
            mine, theirs = halves(value, 2 * bit, place)
            keep, give_low = halves(mine, bit, place)
            give_high, give_both = halves(theirs, bit, place)
            got_both = swap(give_both, 3 * bit, size)
            got_low = swap(give_low, bit, size)
            got_high = swap(give_high, 2 * bit, size)
            value = over(over(keep, got_low, nearer(bit)), over(got_high, got_both, nearer(bit)), nearer(2 * bit))
            bit *= 4
        else:
            value = value.reshape((tiles // 2, 2) + value.shape[1:])
            keep, give = halves(value, bit, place)
            value = over(keep, swap(give, bit, size), nearer(bit))
            bit *= 2
    value = jnp.moveaxis(value[0], 1, 0).reshape(4, rows, width)
    return jnp.concatenate([value[:3], 1.0 - value[3:]], axis=0)


def solution(mesh):
    return jax.shard_map(
        on_device,
        mesh=mesh,
        in_specs=(
            P(("views", "depth"), None, None),
            P("views", "depth", None, None),
            P(("views", "depth"), None, None),
            P("views"),
        ),
        out_specs=P("views", "depth", None),
        check_vma=False,
    )
```

```python
import functools
import math

import jax
import jax.numpy as jnp
from jax import lax
from jax.experimental import pallas as pl
from jax.experimental.pallas import tpu as pltpu
from jax.sharding import PartitionSpec as P


ROWS = 8
CHUNKS = 8
CROSSING = 0xFFFE & ~4


def parity(bits):
    for shift in (8, 4, 2, 1):
        bits = bits ^ (bits >> shift)
    return bits & 1


def side(pair):
    return parity((pair * 2) & CROSSING)


def slot(pair, place, pairs):
    apart = pair ^ (place >> 1)
    quarter = pairs // 4
    return (apart & 3) * quarter + (apart >> 2) if quarter else apart


def march_body(facing, occupied_hbm, dense, emitted, keep, give, dense_buf, emitted_buf, occupied, dense_sem, emitted_sem, small_sem, *, chunks, tile_rows, bricks, ordered):
    depth_len, pairs, _, rows, width = dense.shape
    _, tiles_w = occupied.shape
    per = pairs // chunks
    place = lax.axis_index("depth")
    chosen = (place & 1) ^ side(place >> 1)

    small = pltpu.make_async_copy(occupied_hbm, occupied, small_sem)
    small.start()

    def copies(chunk):
        span = pl.ds(chunk * per, per)
        return (
            pltpu.make_async_copy(dense.at[:, span], dense_buf.at[:, span], dense_sem.at[chunk]),
            pltpu.make_async_copy(emitted.at[:, :, span], emitted_buf.at[:, :, span], emitted_sem.at[chunk]),
        )

    for chunk in range(chunks):
        for copy in copies(chunk):
            copy.start()

    lane = lax.broadcasted_iota(jnp.int32, (ROWS, width), 1) // (width // tiles_w)
    scale = -math.log2(math.e) / (depth_len * bricks)
    small.wait()
    backward = facing[0] != 0

    def march_chunk(chunk, _):
        for copy in copies(chunk):
            copy.wait()

        def march_pair(index, _):
            pair = chunk * per + index
            at = slot(pair, place, pairs) if ordered else pair
            for other, out in ((0, keep), (1, give)):
                half = chosen ^ side(pair) ^ other
                for sub in range(rows // ROWS):
                    tile = ((pair * 2 + half) * rows + sub * ROWS) // tile_rows
                    gate = jnp.zeros((ROWS, width), jnp.float32)
                    for column in range(tiles_w):
                        gate = jnp.where(lane == column, occupied[tile, column].astype(jnp.float32) * scale, gate)
                    span = pl.ds(sub * ROWS, ROWS)
                    total = jnp.zeros((ROWS, width), jnp.float32)
                    before = jnp.ones((ROWS, width), jnp.float32)
                    colour = [jnp.zeros((ROWS, width), jnp.float32) for _ in range(3)]
                    for step in range(depth_len):
                        cell = jnp.where(backward, depth_len - 1 - step, step)
                        total = total + dense_buf[cell, pair, half, span, :]
                        after = jnp.exp2(total * gate)
                        weight = before - after
                        before = after
                        for channel in range(3):
                            colour[channel] = colour[channel] + emitted_buf[channel, cell, pair, half, span, :].astype(jnp.float32) * weight
                    for channel in range(3):
                        out[at, sub, channel] = colour[channel]
                    out[at, sub, 3] = before
            return 0

        lax.fori_loop(0, per, march_pair, 0)
        return 0

    lax.fori_loop(0, chunks, march_chunk, 0)


def march(dense, emitted, occupied, facing, bricks, ordered):
    _, pairs, _, rows, width = dense.shape
    tile_rows = pairs * 2 * rows // occupied.shape[0]
    chunks = math.gcd(pairs, CHUNKS)
    hbm = pl.BlockSpec(memory_space=pl.ANY)
    half = pltpu.VMEM((pairs, rows // ROWS, 4, ROWS, width), jnp.float32)
    return pl.pallas_call(
        functools.partial(march_body, chunks=chunks, tile_rows=tile_rows, bricks=bricks, ordered=ordered),
        in_specs=[pl.BlockSpec(memory_space=pltpu.SMEM), hbm, hbm, hbm],
        out_specs=(pl.BlockSpec(memory_space=pltpu.VMEM), pl.BlockSpec(memory_space=pltpu.VMEM)),
        out_shape=(half, half),
        scratch_shapes=[
            pltpu.VMEM(dense.shape, jnp.float32),
            pltpu.VMEM(emitted.shape, jnp.bfloat16),
            pltpu.SMEM(occupied.shape, jnp.int32),
            pltpu.SemaphoreType.DMA((chunks,)),
            pltpu.SemaphoreType.DMA((chunks,)),
            pltpu.SemaphoreType.DMA,
        ],
        name="march",
    )(facing, occupied, dense, emitted)


def over(mine, other, nearer):
    near, far = jnp.where(nearer, mine, other), jnp.where(nearer, other, mine)
    through = near[3:]
    return jnp.concatenate([near[:3] + through * far[:3], through * far[3:]], axis=0)


def merge(body, facing, arrays, outs):
    def kernel(facing_ref, *refs):
        place = lax.axis_index("depth")
        forward = facing_ref[0] == 0
        body(lambda bit: ((place & bit) == 0) == forward, refs[: len(arrays)], refs[len(arrays) :])

    vmem = pl.BlockSpec(memory_space=pltpu.VMEM)
    return pl.pallas_call(
        kernel,
        in_specs=[pl.BlockSpec(memory_space=pltpu.SMEM)] + [vmem] * len(arrays),
        out_specs=[vmem] * len(outs),
        out_shape=outs,
    )(facing, *(pltpu.with_memory_space_constraint(array, pltpu.VMEM) for array in arrays))


def merge_cores(quarter, nearer, arrays, outs):
    keep, got = arrays
    for index, out in enumerate(outs):
        for k in range(quarter):
            for sub in range(keep.shape[1]):
                at = (index * quarter + k, sub)
                out[k, sub] = over(keep[at], got[at], nearer(1))


def merge_square(bit, nearer, arrays, outs):
    own, low, high, both = arrays
    for k, out in enumerate(outs):
        for sub in range(own.shape[1]):
            first = over(own[k, sub], low[k, sub], nearer(bit))
            second = over(high[k, sub], both[k, sub], nearer(bit))
            out[sub] = over(first, second, nearer(2 * bit))


def merge_pairs(bit, nearer, arrays, outs):
    for k, out in enumerate(outs):
        for sub in range(out.shape[0]):
            out[sub] = over(arrays[2 * k][sub], arrays[2 * k + 1][sub], nearer(bit))


def merge_last(bit, nearer, arrays, outs):
    mine, got = arrays
    for sub in range(mine.shape[0]):
        value = over(mine[sub], got[sub], nearer(bit))
        outs[0][:, pl.ds(sub * mine.shape[2], mine.shape[2]), :] = jnp.concatenate([value[:3], 1.0 - value[3:]], axis=0)


def swap(value, mask, size):
    mask = mask | parity(mask & CROSSING)
    return lax.ppermute(value, "depth", [(i, i ^ mask) for i in range(size)])


def on_device(density, emission, occupancy, facing):
    size = lax.axis_size("depth")
    place = lax.axis_index("depth")
    depth_len, height, width = density.shape
    rows = height // size
    aligned = rows % ROWS == 0
    pairs, unit = (size // 2, rows) if aligned else (height // (2 * ROWS), ROWS)
    dense = density.reshape(depth_len, pairs, 2, unit, width)
    emitted = emission.reshape(3, depth_len, pairs, 2, unit, width)

    keep, give = march(dense, emitted, occupancy[0], facing, size, aligned)
    if not aligned:
        chosen = (place & 1) ^ side(place >> 1)
        pair = jnp.arange(pairs)
        swapped = ((chosen ^ side(pair)) == 1)[:, None, None, None]
        both = jnp.stack([jnp.where(swapped, give[:, 0], keep[:, 0]), jnp.where(swapped, keep[:, 0], give[:, 0])], axis=1)
        pairs = size // 2
        both = jnp.moveaxis(both, 2, 0).reshape(4, pairs, 2, 1, rows, width)
        both = jnp.moveaxis(both, 0, 3)
        pair = jnp.arange(pairs)
        swapped = ((chosen ^ side(pair)) == 1)[:, None, None, None, None]
        order = jnp.zeros((pairs,), jnp.int32).at[slot(pair, place, pairs)].set(pair)
        keep = jnp.where(swapped, both[:, 1], both[:, 0])[order]
        give = jnp.where(swapped, both[:, 0], both[:, 1])[order]
    got = swap(give, 1, size)
    tile = keep.shape[1:]
    quarter = pairs // 4
    group = pltpu.VMEM((quarter,) + tile, jnp.float32)
    own, low, high, both = merge(functools.partial(merge_cores, quarter), facing, (keep, got), [group] * 4)
    got_both = swap(both, 6, size)
    got_low = swap(low, 2, size)
    got_high = swap(high, 4, size)
    one = pltpu.VMEM(tile, jnp.float32)
    mine = merge(functools.partial(merge_square, 2), facing, (own, got_low, got_high, got_both), [one] * quarter)
    bit = 8
    while 2 * bit < size:
        both = [part for k in range(0, len(mine), 2) for part in (mine[k], swap(mine[k + 1], bit, size))]
        mine = merge(functools.partial(merge_pairs, bit), facing, both, [one] * (len(mine) // 2))
        bit *= 2
    image = jax.ShapeDtypeStruct((4, rows, width), jnp.float32)
    return merge(functools.partial(merge_last, bit), facing, (mine[0], swap(mine[1], bit, size)), [image])[0]


def solution(mesh):
    return jax.shard_map(
        on_device,
        mesh=mesh,
        in_specs=(
            P(("views", "depth"), None, None),
            P("views", "depth", None, None),
            P(("views", "depth"), None, None),
            P("views"),
        ),
        out_specs=P("views", "depth", None),
        check_vma=False,
    )
```

```python
import functools
import math

import jax
import jax.numpy as jnp
from jax import lax
from jax.experimental import pallas as pl
from jax.experimental.pallas import tpu as pltpu
from jax.sharding import PartitionSpec as P


ROWS = 8
CHUNKS = 8
SPLIT = ('low', 'high')
ORDER = ('both', 'higha', 'lowa', 'lowb', 'highb')
CROSSING = 0xFFFE & ~4


def parity(bits):
    for shift in (8, 4, 2, 1):
        bits = bits ^ (bits >> shift)
    return bits & 1


def side(pair):
    return parity((pair * 2) & CROSSING)


def slot(pair, place, pairs):
    apart = pair ^ (place >> 1)
    quarter = pairs // 4
    return (apart & 3) * quarter + (apart >> 2) if quarter else apart


def march_body(facing, occupied_hbm, dense, emitted, keep, give, dense_buf, emitted_buf, occupied, dense_sem, emitted_sem, small_sem, *, chunks, tile_rows, bricks, ordered):
    depth_len, pairs, _, rows, width = dense.shape
    _, tiles_w = occupied.shape
    per = pairs // chunks
    place = lax.axis_index("depth")
    chosen = (place & 1) ^ side(place >> 1)

    small = pltpu.make_async_copy(occupied_hbm, occupied, small_sem)
    small.start()

    def copies(chunk):
        span = pl.ds(chunk * per, per)
        return (
            pltpu.make_async_copy(dense.at[:, span], dense_buf.at[:, span], dense_sem.at[chunk]),
            pltpu.make_async_copy(emitted.at[:, :, span], emitted_buf.at[:, :, span], emitted_sem.at[chunk]),
        )

    for chunk in range(chunks):
        for copy in copies(chunk):
            copy.start()

    lane = lax.broadcasted_iota(jnp.int32, (ROWS, width), 1) // (width // tiles_w)
    scale = -math.log2(math.e) / (depth_len * bricks)
    small.wait()
    backward = facing[0] != 0

    def march_chunk(chunk, _):
        for copy in copies(chunk):
            copy.wait()

        def march_pair(index, _):
            pair = chunk * per + index
            at = slot(pair, place, pairs) if ordered else pair
            for other, out in ((0, keep), (1, give)):
                half = chosen ^ side(pair) ^ other
                for sub in range(rows // ROWS):
                    tile = ((pair * 2 + half) * rows + sub * ROWS) // tile_rows
                    gate = jnp.zeros((ROWS, width), jnp.float32)
                    for column in range(tiles_w):
                        gate = jnp.where(lane == column, occupied[tile, column].astype(jnp.float32) * scale, gate)
                    span = pl.ds(sub * ROWS, ROWS)
                    total = jnp.zeros((ROWS, width), jnp.float32)
                    before = jnp.ones((ROWS, width), jnp.float32)
                    colour = [jnp.zeros((ROWS, width), jnp.float32) for _ in range(3)]
                    for step in range(depth_len):
                        cell = jnp.where(backward, depth_len - 1 - step, step)
                        total = total + dense_buf[cell, pair, half, span, :]
                        after = jnp.exp2(total * gate)
                        weight = before - after
                        before = after
                        for channel in range(3):
                            colour[channel] = colour[channel] + emitted_buf[channel, cell, pair, half, span, :].astype(jnp.float32) * weight
                    for channel in range(3):
                        out[at, sub, channel] = colour[channel]
                    out[at, sub, 3] = before
            return 0

        lax.fori_loop(0, per, march_pair, 0)
        return 0

    lax.fori_loop(0, chunks, march_chunk, 0)


def march(dense, emitted, occupied, facing, bricks, ordered):
    _, pairs, _, rows, width = dense.shape
    tile_rows = pairs * 2 * rows // occupied.shape[0]
    chunks = math.gcd(pairs, CHUNKS)
    hbm = pl.BlockSpec(memory_space=pl.ANY)
    half = pltpu.VMEM((pairs, rows // ROWS, 4, ROWS, width), jnp.float32)
    return pl.pallas_call(
        functools.partial(march_body, chunks=chunks, tile_rows=tile_rows, bricks=bricks, ordered=ordered),
        in_specs=[pl.BlockSpec(memory_space=pltpu.SMEM), hbm, hbm, hbm],
        out_specs=(pl.BlockSpec(memory_space=pltpu.VMEM), pl.BlockSpec(memory_space=pltpu.VMEM)),
        out_shape=(half, half),
        scratch_shapes=[
            pltpu.VMEM(dense.shape, jnp.float32),
            pltpu.VMEM(emitted.shape, jnp.bfloat16),
            pltpu.SMEM(occupied.shape, jnp.int32),
            pltpu.SemaphoreType.DMA((chunks,)),
            pltpu.SemaphoreType.DMA((chunks,)),
            pltpu.SemaphoreType.DMA,
        ],
        name="march",
    )(facing, occupied, dense, emitted)


def over(mine, other, nearer):
    near, far = jnp.where(nearer, mine, other), jnp.where(nearer, other, mine)
    through = near[3:]
    return jnp.concatenate([near[:3] + through * far[:3], through * far[3:]], axis=0)


def merge(body, facing, arrays, outs):
    def kernel(facing_ref, *refs):
        place = lax.axis_index("depth")
        forward = facing_ref[0] == 0
        body(lambda bit: ((place & bit) == 0) == forward, refs[: len(arrays)], refs[len(arrays) :])

    vmem = pl.BlockSpec(memory_space=pltpu.VMEM)
    return pl.pallas_call(
        kernel,
        in_specs=[pl.BlockSpec(memory_space=pltpu.SMEM)] + [vmem] * len(arrays),
        out_specs=[vmem] * len(outs),
        out_shape=outs,
    )(facing, *(pltpu.with_memory_space_constraint(array, pltpu.VMEM) for array in arrays))


def merge_cores(groups, nearer, arrays, outs):
    keep, got = arrays
    for group, out in zip(groups, outs):
        for k, at in enumerate(group):
            for sub in range(keep.shape[1]):
                out[k, sub] = over(keep[at, sub], got[at, sub], nearer(1))


def merge_square(bit, nearer, arrays, outs):
    for k, out in enumerate(outs):
        own, low, high, both = ((ref, at) for ref, at in zip(arrays, bit[1][k]))
        for sub in range(out.shape[0]):
            first = over(own[0][own[1], sub], low[0][low[1], sub], nearer(bit[0]))
            second = over(high[0][high[1], sub], both[0][both[1], sub], nearer(bit[0]))
            out[sub] = over(first, second, nearer(2 * bit[0]))


def merge_pairs(bit, nearer, arrays, outs):
    for k, out in enumerate(outs):
        for sub in range(out.shape[0]):
            out[sub] = over(arrays[2 * k][sub], arrays[2 * k + 1][sub], nearer(bit))


def merge_last(bit, nearer, arrays, outs):
    mine, got = arrays
    for sub in range(mine.shape[0]):
        value = over(mine[sub], got[sub], nearer(bit))
        outs[0][:, pl.ds(sub * mine.shape[2], mine.shape[2]), :] = jnp.concatenate([value[:3], 1.0 - value[3:]], axis=0)


def swap(value, mask, size):
    mask = mask | parity(mask & CROSSING)
    return lax.ppermute(value, "depth", [(i, i ^ mask) for i in range(size)])


def on_device(density, emission, occupancy, facing):
    size = lax.axis_size("depth")
    place = lax.axis_index("depth")
    depth_len, height, width = density.shape
    rows = height // size
    aligned = rows % ROWS == 0
    pairs, unit = (size // 2, rows) if aligned else (height // (2 * ROWS), ROWS)
    dense = density.reshape(depth_len, pairs, 2, unit, width)
    emitted = emission.reshape(3, depth_len, pairs, 2, unit, width)

    keep, give = march(dense, emitted, occupancy[0], facing, size, aligned)
    if not aligned:
        chosen = (place & 1) ^ side(place >> 1)
        pair = jnp.arange(pairs)
        swapped = ((chosen ^ side(pair)) == 1)[:, None, None, None]
        both = jnp.stack([jnp.where(swapped, give[:, 0], keep[:, 0]), jnp.where(swapped, keep[:, 0], give[:, 0])], axis=1)
        pairs = size // 2
        both = jnp.moveaxis(both, 2, 0).reshape(4, pairs, 2, 1, rows, width)
        both = jnp.moveaxis(both, 0, 3)
        pair = jnp.arange(pairs)
        swapped = ((chosen ^ side(pair)) == 1)[:, None, None, None, None]
        order = jnp.zeros((pairs,), jnp.int32).at[slot(pair, place, pairs)].set(pair)
        keep = jnp.where(swapped, both[:, 1], both[:, 0])[order]
        give = jnp.where(swapped, both[:, 0], both[:, 1])[order]
    got = swap(give, 1, size)
    tile = keep.shape[1:]
    quarter = pairs // 4
    later, sooner = list(range(0, quarter, 2)), list(range(1, quarter, 2))
    groups = {}
    for index, name in enumerate(("own", "low", "high", "both")):
        for part, members in (("a", sooner), ("b", later)) if name in SPLIT else (("", sooner + later),):
            groups[name + part] = [index * quarter + k for k in members]
    shapes = [pltpu.VMEM((len(group),) + tile, jnp.float32) for group in groups.values()]
    parts = merge(functools.partial(merge_cores, list(groups.values())), facing, (keep, got), shapes)
    parts = dict(zip(groups, parts))
    arrived = {"own": parts["own"]}
    for name in ORDER:
        arrived[name] = swap(parts[name], {"low": 2, "high": 4, "both": 6}[name.rstrip("ab") if name != "both" else name], size)
    one = pltpu.VMEM(tile, jnp.float32)

    def square(members, part):
        names = [name + (part if name in SPLIT else "") for name in ("own", "low", "high", "both")]
        places = [[groups[name].index(index * quarter + k) for index, name in enumerate(names)] for k in members]
        return merge(functools.partial(merge_square, (2, places)), facing, [arrived[name] for name in names], [one] * len(members))

    going, staying = square(sooner, "a"), square(later, "b")
    mine = [part for pair in zip(staying, going) for part in pair]
    bit = 8
    while 2 * bit < size:
        both = [part for k in range(0, len(mine), 2) for part in (mine[k], swap(mine[k + 1], bit, size))]
        mine = merge(functools.partial(merge_pairs, bit), facing, both, [one] * (len(mine) // 2))
        bit *= 2
    image = jax.ShapeDtypeStruct((4, rows, width), jnp.float32)
    got = swap(mine[1], bit, size)
    return merge(functools.partial(merge_last, bit), facing, (mine[0], got), [image])[0]


def solution(mesh):
    return jax.shard_map(
        on_device,
        mesh=mesh,
        in_specs=(
            P(("views", "depth"), None, None),
            P("views", "depth", None, None),
            P(("views", "depth"), None, None),
            P("views"),
        ),
        out_specs=P("views", "depth", None),
        check_vma=False,
    )
```

```python
import functools
import math

import jax
import jax.numpy as jnp
from jax import lax
from jax.experimental import pallas as pl
from jax.experimental.pallas import tpu as pltpu
from jax.sharding import PartitionSpec as P


ROWS = 8
LANES = 128
BOUNDS = (0, 1, 2, 3, 4, 5, 6, 7, 8)
SPLIT = ('low', 'high')
ORDER = ('both', 'higha', 'lowa', 'lowb', 'highb')
CROSSING = 0xFFFE & ~4


def parity(bits):
    for shift in (8, 4, 2, 1):
        bits = bits ^ (bits >> shift)
    return bits & 1


def side(pair):
    return parity((pair * 2) & CROSSING)


def slot(pair, place, pairs):
    apart = pair ^ (place >> 1)
    quarter = pairs // 4
    return (apart & 3) * quarter + (apart >> 2) if quarter else apart


def march_body(occupied_hbm, dense, emitted, keep, give, dense_buf, emitted_buf, occupied, dense_sem, emitted_sem, small_sem, *, bounds, tile_rows, bricks, ordered):
    depth_len, pairs, _, rows, width = dense.shape
    _, tiles_w = occupied.shape
    place = lax.axis_index("depth")
    chosen = (place & 1) ^ side(place >> 1)

    small = pltpu.make_async_copy(occupied_hbm, occupied, small_sem)
    small.start()

    def copies(chunk):
        span = pl.ds(bounds[chunk], bounds[chunk + 1] - bounds[chunk])
        return (
            pltpu.make_async_copy(dense.at[:, span], dense_buf.at[:, span], dense_sem.at[chunk]),
            pltpu.make_async_copy(emitted.at[:, :, span], emitted_buf.at[:, :, span], emitted_sem.at[chunk]),
        )

    for chunk in range(len(bounds) - 1):
        for copy in copies(chunk):
            copy.start()

    lane = lax.broadcasted_iota(jnp.int32, (ROWS, width), 1) // (width // tiles_w)
    scale = -math.log2(math.e) / (depth_len * bricks)
    small.wait()

    def march_tile(pair, other, out):
        at = slot(pair, place, pairs) if ordered else pair
        half = chosen ^ side(pair) ^ other
        for sub in range(rows // ROWS):
            tile = ((pair * 2 + half) * rows + sub * ROWS) // tile_rows
            gates = jnp.zeros((ROWS, width), jnp.float32)
            for column in range(tiles_w):
                gates = jnp.where(lane == column, occupied[tile, column].astype(jnp.float32) * scale, gates)
            span = pl.ds(sub * ROWS, ROWS)
            for left in range(0, width, LANES):
                lanes = pl.ds(left, LANES)
                gate = gates[:, left : left + LANES]
                total = jnp.zeros((ROWS, LANES), jnp.float32)
                through = inverse = jnp.ones((ROWS, LANES), jnp.float32)
                fore = [jnp.zeros((ROWS, LANES), jnp.float32) for _ in range(3)]
                back = [jnp.zeros((ROWS, LANES), jnp.float32) for _ in range(3)]
                for cell in range(depth_len):
                    total = total + dense_buf[cell, pair, half, span, lanes]
                    depth = total * gate
                    through, last = jnp.exp2(depth), through
                    inverse, last_inverse = jnp.exp2(-depth), inverse
                    for channel in range(3):
                        colour = emitted_buf[channel, cell, pair, half, span, lanes].astype(jnp.float32)
                        fore[channel] = fore[channel] + colour * (last - through)
                        back[channel] = back[channel] + colour * (inverse - last_inverse)
                for channel in range(3):
                    out[at, sub, channel, :, lanes] = fore[channel]
                    out[at, sub, 4 + channel, :, lanes] = back[channel] * through
                out[at, sub, 3, :, lanes] = through

    for chunk in range(len(bounds) - 1):
        for copy in copies(chunk):
            copy.wait()

        def march_pair(pair, _):
            for other, out in ((0, keep), (1, give)):
                march_tile(pair, other, out)
            return 0

        lax.fori_loop(bounds[chunk], bounds[chunk + 1], march_pair, 0)


def march(dense, emitted, occupied, bricks, ordered):
    _, pairs, _, rows, width = dense.shape
    tile_rows = pairs * 2 * rows // occupied.shape[0]
    bounds = [pairs * eighth // 8 for eighth in BOUNDS] if pairs % 8 == 0 else [0, pairs]
    chunks = len(bounds) - 1
    hbm = pl.BlockSpec(memory_space=pl.ANY)
    half = pltpu.VMEM((pairs, rows // ROWS, 7, ROWS, width), jnp.float32)
    return pl.pallas_call(
        functools.partial(march_body, bounds=bounds, tile_rows=tile_rows, bricks=bricks, ordered=ordered),
        in_specs=[hbm, hbm, hbm],
        out_specs=(pl.BlockSpec(memory_space=pltpu.VMEM), pl.BlockSpec(memory_space=pltpu.VMEM)),
        out_shape=(half, half),
        scratch_shapes=[
            pltpu.VMEM(dense.shape, jnp.float32),
            pltpu.VMEM(emitted.shape, jnp.bfloat16),
            pltpu.SMEM(occupied.shape, jnp.int32),
            pltpu.SemaphoreType.DMA((chunks,)),
            pltpu.SemaphoreType.DMA((chunks,)),
            pltpu.SemaphoreType.DMA,
        ],
        name="march",
    )(occupied, dense, emitted)


def over(mine, other, nearer):
    near, far = jnp.where(nearer, mine, other), jnp.where(nearer, other, mine)
    through = near[3:]
    return jnp.concatenate([near[:3] + through * far[:3], through * far[3:]], axis=0)


def merge(body, facing, arrays, outs):
    def kernel(facing_ref, *refs):
        place = lax.axis_index("depth")
        forward = facing_ref[0] == 0
        body(lambda bit: ((place & bit) == 0) == forward, refs[: len(arrays)], refs[len(arrays) :])

    vmem = pl.BlockSpec(memory_space=pltpu.VMEM)
    return pl.pallas_call(
        kernel,
        in_specs=[pl.BlockSpec(memory_space=pltpu.SMEM)] + [vmem] * len(arrays),
        out_specs=[vmem] * len(outs),
        out_shape=outs,
    )(facing, *(pltpu.with_memory_space_constraint(array, pltpu.VMEM) for array in arrays))


def merge_cores(groups, nearer, arrays, outs):
    keep, got = arrays
    forward = nearer(0)

    def seen(tile):
        return jnp.concatenate([jnp.where(forward, tile[:3], tile[4:]), tile[3:4]], axis=0)

    for group, out in zip(groups, outs):
        for k, at in enumerate(group):
            for sub in range(keep.shape[1]):
                out[k, sub] = over(seen(keep[at, sub]), seen(got[at, sub]), nearer(1))


def merge_square(bit, nearer, arrays, outs):
    for k, out in enumerate(outs):
        own, low, high, both = ((ref, at) for ref, at in zip(arrays, bit[1][k]))
        for sub in range(out.shape[0]):
            first = over(own[0][own[1], sub], low[0][low[1], sub], nearer(bit[0]))
            second = over(high[0][high[1], sub], both[0][both[1], sub], nearer(bit[0]))
            out[sub] = over(first, second, nearer(2 * bit[0]))


def merge_pairs(bit, nearer, arrays, outs):
    for k, out in enumerate(outs):
        for sub in range(out.shape[0]):
            out[sub] = over(arrays[2 * k][sub], arrays[2 * k + 1][sub], nearer(bit))


def merge_last(bit, nearer, arrays, outs):
    mine, got = arrays
    for sub in range(mine.shape[0]):
        value = over(mine[sub], got[sub], nearer(bit))
        outs[0][:, pl.ds(sub * mine.shape[2], mine.shape[2]), :] = jnp.concatenate([value[:3], 1.0 - value[3:]], axis=0)


def swap(value, mask, size):
    mask = mask | parity(mask & CROSSING)
    return lax.ppermute(value, "depth", [(i, i ^ mask) for i in range(size)])


def on_device(density, emission, occupancy, facing):
    size = lax.axis_size("depth")
    place = lax.axis_index("depth")
    depth_len, height, width = density.shape
    rows = height // size
    aligned = rows % ROWS == 0
    pairs, unit = (size // 2, rows) if aligned else (height // (2 * ROWS), ROWS)
    dense = density.reshape(depth_len, pairs, 2, unit, width)
    emitted = emission.reshape(3, depth_len, pairs, 2, unit, width)

    keep, give = march(dense, emitted, occupancy[0], size, aligned)
    if not aligned:
        chosen = (place & 1) ^ side(place >> 1)
        pair = jnp.arange(pairs)
        swapped = ((chosen ^ side(pair)) == 1)[:, None, None, None]
        both = jnp.stack([jnp.where(swapped, give[:, 0], keep[:, 0]), jnp.where(swapped, keep[:, 0], give[:, 0])], axis=1)
        pairs = size // 2
        both = jnp.moveaxis(both, 2, 0).reshape(7, pairs, 2, 1, rows, width)
        both = jnp.moveaxis(both, 0, 3)
        pair = jnp.arange(pairs)
        swapped = ((chosen ^ side(pair)) == 1)[:, None, None, None, None]
        order = jnp.zeros((pairs,), jnp.int32).at[slot(pair, place, pairs)].set(pair)
        keep = jnp.where(swapped, both[:, 1], both[:, 0])[order]
        give = jnp.where(swapped, both[:, 0], both[:, 1])[order]
    got = swap(give, 1, size)
    tile = (keep.shape[1], 4) + keep.shape[3:]
    quarter = pairs // 4
    later, sooner = list(range(0, quarter, 2)), list(range(1, quarter, 2))
    groups = {}
    for index, name in enumerate(("own", "low", "high", "both")):
        for part, members in (("a", sooner), ("b", later)) if name in SPLIT else (("", sooner + later),):
            groups[name + part] = [index * quarter + k for k in members]
    shapes = [pltpu.VMEM((len(group),) + tile, jnp.float32) for group in groups.values()]
    parts = merge(functools.partial(merge_cores, list(groups.values())), facing, (keep, got), shapes)
    parts = dict(zip(groups, parts))
    arrived = {"own": parts["own"]}
    for name in ORDER:
        arrived[name] = swap(parts[name], {"low": 2, "high": 4, "both": 6}[name.rstrip("ab") if name != "both" else name], size)
    one = pltpu.VMEM(tile, jnp.float32)

    def square(members, part):
        names = [name + (part if name in SPLIT else "") for name in ("own", "low", "high", "both")]
        places = [[groups[name].index(index * quarter + k) for index, name in enumerate(names)] for k in members]
        return merge(functools.partial(merge_square, (2, places)), facing, [arrived[name] for name in names], [one] * len(members))

    going, staying = square(sooner, "a"), square(later, "b")
    mine = [part for pair in zip(staying, going) for part in pair]
    bit = 8
    while 2 * bit < size:
        both = [part for k in range(0, len(mine), 2) for part in (mine[k], swap(mine[k + 1], bit, size))]
        mine = merge(functools.partial(merge_pairs, bit), facing, both, [one] * (len(mine) // 2))
        bit *= 2
    image = jax.ShapeDtypeStruct((4, rows, width), jnp.float32)
    got = swap(mine[1], bit, size)
    return merge(functools.partial(merge_last, bit), facing, (mine[0], got), [image])[0]


def solution(mesh):
    return jax.shard_map(
        on_device,
        mesh=mesh,
        in_specs=(
            P(("views", "depth"), None, None),
            P("views", "depth", None, None),
            P(("views", "depth"), None, None),
            P("views"),
        ),
        out_specs=P("views", "depth", None),
        check_vma=False,
    )
```

```python
import functools
import math

import jax
import jax.numpy as jnp
from jax import lax
from jax.experimental import pallas as pl
from jax.experimental.pallas import tpu as pltpu
from jax.sharding import PartitionSpec as P


ROWS = 8
LANES = 128
BOUNDS = (0, 1, 2, 3, 4, 5, 6, 7, 8)
QUARTERS = {"own": (0, 0), "turn": (1, 2), "back": (2, 1), "across": (3, 3)}
SPLIT = ("turn", "back")
ORDER = ("across", "turna", "backa", "backb", "turnb")
CROSSING = 0xFFFE


def parity(bits):
    for shift in (8, 4, 2, 1):
        bits = bits ^ (bits >> shift)
    return bits & 1


def side(pair):
    return parity((pair * 2) & CROSSING)


def slot(pair, place, pairs):
    apart = pair ^ (place >> 1)
    quarter = pairs // 4
    return (apart & 3) * quarter + (apart >> 2) if quarter else apart


def march_body(occupied_hbm, dense, emitted, keep, give, dense_buf, emitted_buf, occupied, dense_sem, emitted_sem, small_sem, *, bounds, tile_rows, bricks, ordered):
    depth_len, pairs, _, rows, width = dense.shape
    _, tiles_w = occupied.shape
    place = lax.axis_index("depth")
    chosen = (place & 1) ^ side(place >> 1)

    small = pltpu.make_async_copy(occupied_hbm, occupied, small_sem)
    small.start()

    def copies(chunk):
        span = pl.ds(bounds[chunk], bounds[chunk + 1] - bounds[chunk])
        return (
            pltpu.make_async_copy(dense.at[:, span], dense_buf.at[:, span], dense_sem.at[chunk]),
            pltpu.make_async_copy(emitted.at[:, :, span], emitted_buf.at[:, :, span], emitted_sem.at[chunk]),
        )

    for chunk in range(len(bounds) - 1):
        for copy in copies(chunk):
            copy.start()

    lane = lax.broadcasted_iota(jnp.int32, (ROWS, width), 1) // (width // tiles_w)
    scale = -math.log2(math.e) / (depth_len * bricks)
    small.wait()

    def march_tile(pair, other, out):
        at = slot(pair, place, pairs) if ordered else pair
        half = chosen ^ side(pair) ^ other
        for sub in range(rows // ROWS):
            tile = ((pair * 2 + half) * rows + sub * ROWS) // tile_rows
            gates = jnp.zeros((ROWS, width), jnp.float32)
            for column in range(tiles_w):
                gates = jnp.where(lane == column, occupied[tile, column].astype(jnp.float32) * scale, gates)
            span = pl.ds(sub * ROWS, ROWS)
            for left in range(0, width, LANES):
                lanes = pl.ds(left, LANES)
                gate = gates[:, left : left + LANES]
                total = jnp.zeros((ROWS, LANES), jnp.float32)
                through = inverse = jnp.ones((ROWS, LANES), jnp.float32)
                fore = [jnp.zeros((ROWS, LANES), jnp.float32) for _ in range(3)]
                back = [jnp.zeros((ROWS, LANES), jnp.float32) for _ in range(3)]
                for cell in range(depth_len):
                    total = total + dense_buf[cell, pair, half, span, lanes]
                    depth = total * gate
                    through, last = jnp.exp2(depth), through
                    inverse, last_inverse = jnp.exp2(-depth), inverse
                    for channel in range(3):
                        colour = emitted_buf[channel, cell, pair, half, span, lanes].astype(jnp.float32)
                        fore[channel] = fore[channel] + colour * (last - through)
                        back[channel] = back[channel] + colour * (inverse - last_inverse)
                for channel in range(3):
                    out[at, sub, channel, :, lanes] = fore[channel]
                    out[at, sub, 4 + channel, :, lanes] = back[channel] * through
                out[at, sub, 3, :, lanes] = through

    for chunk in range(len(bounds) - 1):
        for copy in copies(chunk):
            copy.wait()

        def march_pair(pair, _):
            for other, out in ((0, keep), (1, give)):
                march_tile(pair, other, out)
            return 0

        lax.fori_loop(bounds[chunk], bounds[chunk + 1], march_pair, 0)


def march(dense, emitted, occupied, bricks, ordered):
    _, pairs, _, rows, width = dense.shape
    tile_rows = pairs * 2 * rows // occupied.shape[0]
    bounds = [pairs * eighth // 8 for eighth in BOUNDS] if pairs % 8 == 0 else [0, pairs]
    chunks = len(bounds) - 1
    hbm = pl.BlockSpec(memory_space=pl.ANY)
    half = pltpu.VMEM((pairs, rows // ROWS, 7, ROWS, width), jnp.float32)
    return pl.pallas_call(
        functools.partial(march_body, bounds=bounds, tile_rows=tile_rows, bricks=bricks, ordered=ordered),
        in_specs=[hbm, hbm, hbm],
        out_specs=(pl.BlockSpec(memory_space=pltpu.VMEM), pl.BlockSpec(memory_space=pltpu.VMEM)),
        out_shape=(half, half),
        scratch_shapes=[
            pltpu.VMEM(dense.shape, jnp.float32),
            pltpu.VMEM(emitted.shape, jnp.bfloat16),
            pltpu.SMEM(occupied.shape, jnp.int32),
            pltpu.SemaphoreType.DMA((chunks,)),
            pltpu.SemaphoreType.DMA((chunks,)),
            pltpu.SemaphoreType.DMA,
        ],
        name="march",
    )(occupied, dense, emitted)


def over(mine, other, nearer):
    near, far = jnp.where(nearer, mine, other), jnp.where(nearer, other, mine)
    through = near[3:]
    return jnp.concatenate([near[:3] + through * far[:3], through * far[3:]], axis=0)


def merge(body, facing, arrays, outs):
    def kernel(facing_ref, *refs):
        place = lax.axis_index("depth")
        forward = facing_ref[0] == 0
        body(lambda bit: ((place & bit) == 0) == forward, refs[: len(arrays)], refs[len(arrays) :])

    vmem = pl.BlockSpec(memory_space=pltpu.VMEM)
    return pl.pallas_call(
        kernel,
        in_specs=[pl.BlockSpec(memory_space=pltpu.SMEM)] + [vmem] * len(arrays),
        out_specs=[vmem] * len(outs),
        out_shape=outs,
    )(facing, *(pltpu.with_memory_space_constraint(array, pltpu.VMEM) for array in arrays))


def merge_cores(groups, nearer, arrays, outs):
    keep, got = arrays
    forward = nearer(0)

    def seen(tile):
        return jnp.concatenate([jnp.where(forward, tile[:3], tile[4:]), tile[3:4]], axis=0)

    quarter = keep.shape[0] // 4
    odd = parity((lax.axis_index("depth") >> 1) & 3)
    for (even_quarter, odd_quarter, members), out in zip(groups, outs):
        start = even_quarter * quarter if even_quarter == odd_quarter else jnp.where(odd == 1, odd_quarter, even_quarter) * quarter
        for k, at in enumerate(members):
            for sub in range(keep.shape[1]):
                out[k, sub] = over(seen(keep[start + at, sub]), seen(got[start + at, sub]), nearer(1))


def merge_square(bit, nearer, arrays, outs):
    odd = parity((lax.axis_index("depth") >> 1) & 3) == 1
    for k, out in enumerate(outs):
        own, turn, back, both = ((ref, at) for ref, at in zip(arrays, bit[1][k]))
        for sub in range(out.shape[0]):
            turned, returned = turn[0][turn[1], sub], back[0][back[1], sub]
            low, high = jnp.where(odd, turned, returned), jnp.where(odd, returned, turned)
            first = over(own[0][own[1], sub], low, nearer(bit[0]))
            second = over(high, both[0][both[1], sub], nearer(bit[0]))
            out[sub] = over(first, second, nearer(2 * bit[0]))


def merge_pairs(bit, nearer, arrays, outs):
    for k, out in enumerate(outs):
        for sub in range(out.shape[0]):
            out[sub] = over(arrays[2 * k][sub], arrays[2 * k + 1][sub], nearer(bit))


def merge_last(bit, nearer, arrays, outs):
    mine, got = arrays
    for sub in range(mine.shape[0]):
        value = over(mine[sub], got[sub], nearer(bit))
        outs[0][:, pl.ds(sub * mine.shape[2], mine.shape[2]), :] = jnp.concatenate([value[:3], 1.0 - value[3:]], axis=0)


def swap(value, masks, size):
    even, odd = (mask | parity(mask & CROSSING) for mask in (masks if isinstance(masks, list) else [masks, masks]))
    return lax.ppermute(value, "depth", [(i, i ^ (odd if parity((i >> 1) & 3) else even)) for i in range(size)])


def on_device(density, emission, occupancy, facing):
    size = lax.axis_size("depth")
    place = lax.axis_index("depth")
    depth_len, height, width = density.shape
    rows = height // size
    aligned = rows % ROWS == 0
    pairs, unit = (size // 2, rows) if aligned else (height // (2 * ROWS), ROWS)
    dense = density.reshape(depth_len, pairs, 2, unit, width)
    emitted = emission.reshape(3, depth_len, pairs, 2, unit, width)

    keep, give = march(dense, emitted, occupancy[0], size, aligned)
    if not aligned:
        chosen = (place & 1) ^ side(place >> 1)
        pair = jnp.arange(pairs)
        swapped = ((chosen ^ side(pair)) == 1)[:, None, None, None]
        both = jnp.stack([jnp.where(swapped, give[:, 0], keep[:, 0]), jnp.where(swapped, keep[:, 0], give[:, 0])], axis=1)
        pairs = size // 2
        both = jnp.moveaxis(both, 2, 0).reshape(7, pairs, 2, 1, rows, width)
        both = jnp.moveaxis(both, 0, 3)
        pair = jnp.arange(pairs)
        swapped = ((chosen ^ side(pair)) == 1)[:, None, None, None, None]
        order = jnp.zeros((pairs,), jnp.int32).at[slot(pair, place, pairs)].set(pair)
        keep = jnp.where(swapped, both[:, 1], both[:, 0])[order]
        give = jnp.where(swapped, both[:, 0], both[:, 1])[order]
    got = swap(give, 1, size)
    tile = (keep.shape[1], 4) + keep.shape[3:]
    quarter = pairs // 4
    later, sooner = list(range(0, quarter, 2)), list(range(1, quarter, 2))
    groups = {}
    for name, (even_quarter, odd_quarter) in QUARTERS.items():
        for part, members in (("a", sooner), ("b", later)) if name in SPLIT else (("", sooner + later),):
            groups[name + part] = (even_quarter, odd_quarter, members)
    shapes = [pltpu.VMEM((len(members),) + tile, jnp.float32) for _, _, members in groups.values()]
    parts = merge(functools.partial(merge_cores, list(groups.values())), facing, (keep, got), shapes)
    parts = dict(zip(groups, parts))
    arrived = {"own": parts["own"]}
    for name in ORDER:
        arrived[name] = swap(parts[name], [2 * quarter_of for quarter_of in groups[name][:2]], size)
    one = pltpu.VMEM(tile, jnp.float32)

    def square(members, part):
        names = [name + (part if name in SPLIT else "") for name in QUARTERS]
        places = [[groups[name][2].index(k) for name in names] for k in members]
        return merge(functools.partial(merge_square, (2, places)), facing, [arrived[name] for name in names], [one] * len(members))

    going, staying = square(sooner, "a"), square(later, "b")
    mine = [part for pair in zip(staying, going) for part in pair]
    bit = 8
    while 2 * bit < size:
        both = [part for k in range(0, len(mine), 2) for part in (mine[k], swap(mine[k + 1], bit, size))]
        mine = merge(functools.partial(merge_pairs, bit), facing, both, [one] * (len(mine) // 2))
        bit *= 2
    image = jax.ShapeDtypeStruct((4, rows, width), jnp.float32)
    got = swap(mine[1], bit, size)
    return merge(functools.partial(merge_last, bit), facing, (mine[0], got), [image])[0]


def solution(mesh):
    return jax.shard_map(
        on_device,
        mesh=mesh,
        in_specs=(
            P(("views", "depth"), None, None),
            P("views", "depth", None, None),
            P(("views", "depth"), None, None),
            P("views"),
        ),
        out_specs=P("views", "depth", None),
        check_vma=False,
    )
```
